32 devices in a mesh: dp: 16 (over z, y, core), local: 2 (over x).
Axes of the slice: x: 2, y: 2, z: 4, core: 2. Of those that a mesh axis runs over, the one named last changes fastest.
Arguments:
- pre_glu: bfloat16 [32, 256, 3072], P(('dp', 'local')), may hold values from -80 to 80
- lengths: int32 [32], P(('dp', 'local')), may hold values from 1 to 256, as said below
- kernel: float32 [5, 1536], replicated, may hold values from -2.5 to 2.5
- bn_gain: float32 [1536], replicated, may hold values from 0.5 to 2
- bn_shift: float32 [1536], replicated, may hold values from -1 to 1
- w_out: bfloat16 [1536, 1536], replicated, may hold values from -0.15625 to 0.15625
- cotangent: bfloat16 [32, 256, 1536], P(('dp', 'local')), may hold values from -6 to 6
Outputs:
- grad_pre_glu: bfloat16 [32, 256, 3072], P(('dp', 'local'))
- grad_w_out: float32 [1536, 1536], P('dp', 'local')
- grad_kernel: float32 [5, 1536], replicated
- grad_gain: float32 [1536], replicated
- grad_shift: float32 [1536], replicated
The draws below stay inside these ranges and needn't reach their ends.
Inputs may be any that keep to these rules, and one draw needn't show every extreme that they name: `lengths`: each utterance's valid frames are its first ones; some utterance has all 256 frames valid.
All inputs are finite; a program needn't handle non-finite values.
Results may differ from the reference program's by a relative error of at most 0.0029.
Values sent between devices are 32-bit elements; how exact they have to be, the bound alone decides.
No kernel may reach another device: no remote copies, remote signals or barrier semaphores. Data moves between devices by JAX's collectives and lax.ppermute only.
A program may use at most 64 MiB of HBM per device.

```python
import math
import jax
import jax.numpy as jnp
from jax import lax

WIDTH = 1536
TAPS = 5
FRAMES = 256
UTTERANCES = 32


def draw_pre_glu(key, part):
    key_a, key_b, key_c = jax.random.split(key, 3)
    ranks = jnp.arange(UTTERANCES, dtype=jnp.float32) / max(UTTERANCES - 1, 1)
    chan_scale = jnp.exp(jax.random.uniform(key_b, (2 * WIDTH,), jnp.float32, jnp.log(0.3), jnp.log(3.0)))
    offsets = 0.5 * jnp.clip(jax.random.normal(key_c, (2 * WIDTH,), jnp.float32), -4.0, 4.0)
    row_scale = 3.0 ** ranks
    base_draw = jnp.clip(jax.random.normal(key_a, (UTTERANCES, FRAMES, 2 * WIDTH), jnp.float32), -4.0, 4.0)
    values = base_draw * row_scale[:, None, None] * chan_scale + ranks[:, None, None] * offsets
    return values.astype(jnp.bfloat16)


def draw_lengths(key, part):
    ranks = jnp.arange(UTTERANCES, dtype=jnp.int32)
    floor_len = FRAMES // 3 + ranks * (FRAMES - FRAMES // 3) // max(UTTERANCES - 1, 1)
    jitter = jax.random.randint(key, (UTTERANCES,), 0, FRAMES // 8 + 1, dtype=jnp.int32)
    values = jnp.clip(floor_len - jitter, 1, FRAMES)
    return jnp.where(ranks == UTTERANCES - 1, FRAMES, values).astype(jnp.int32)


def shard_levels(stream_key, dims, pieces, smallest, high):
    def one(axis_at, shards_of):
        heights = jax.random.uniform(jax.random.fold_in(jax.random.fold_in(stream_key, 6), axis_at), (shards_of,), jnp.float32, smallest / len(pieces), high / len(pieces))
        return jnp.repeat(jnp.exp(heights), dims[axis_at] // shards_of).reshape((-1,) + (1,) * (len(dims) - axis_at - 1))

    level = one(*pieces[0])
    for cut in pieces[1:]:
        level = level * one(*cut)
    return level


def gaussian(key, extent, spread, reach, cuts=(), kind=jnp.bfloat16):
    array = spread * jax.random.normal(key, extent, jnp.float32)
    if cuts:
        array = array * shard_levels(key, extent, cuts, -0.22, 0.18)
    return jnp.clip(array, -reach, reach).astype(kind)


def setup_inputs(seed: int = 0) -> dict:
    seeds = jax.random.split(jax.random.key(seed), 8)
    return {
        "pre_glu": draw_pre_glu(jax.random.fold_in(seeds[7], 71), 0),
        "lengths": draw_lengths(jax.random.fold_in(seeds[7], 71), 0),
        "kernel": gaussian(seeds[2], (TAPS, WIDTH), TAPS ** -0.5, 2.5, (), jnp.float32),
        "bn_gain": jnp.clip(jnp.exp(jax.random.uniform(seeds[3], (WIDTH,), jnp.float32, math.log(0.5), math.log(2.0))), 0.5, 2.0),
        "bn_shift": jnp.clip(jax.random.uniform(seeds[4], (WIDTH,), jnp.float32, -1.0, 1.0), -1.0, 1.0),
        "w_out": gaussian(seeds[5], (WIDTH, WIDTH), WIDTH ** -0.5, 0.15625),
        "cotangent": gaussian(seeds[6], (UTTERANCES, FRAMES, WIDTH), 1.0, 6.0, ((0, 32),)),
    }


epsilon = 1e-05

def front_pass(pre_one, length, kernel):
    frames = pre_one.shape[0]
    model_width = kernel.shape[1]
    kernel_taps = kernel.shape[0]
    half_width = (kernel_taps - 1) // 2
    valid_mask = (jnp.arange(frames, dtype=jnp.int32)[:, None] < length).astype(jnp.float32)
    first_half = pre_one[:, :model_width].astype(jnp.float32)
    gate_value = jax.nn.sigmoid(pre_one[:, model_width:].astype(jnp.float32))
    glu_out = first_half * gate_value * valid_mask
    padded = jnp.pad(glu_out, ((half_width, half_width), (0, 0)))
    conv_out = kernel[0] * padded[0:frames]
    for j in range(1, kernel_taps):
        conv_out = conv_out + kernel[j] * padded[j:j + frames]
    return (valid_mask, first_half, gate_value, padded, conv_out)

def reference(pre_glu, lengths, kernel, bn_gain, bn_shift, w_out, cotangent):
    replicas = pre_glu.shape[0]
    frames = pre_glu.shape[1]
    model_width = kernel.shape[1]
    kernel_taps = kernel.shape[0]
    half_width = (kernel_taps - 1) // 2
    frame_total = jnp.sum(lengths).astype(jnp.float32)
    zeros_row = jnp.zeros((model_width,), jnp.float32)

    def mean_step(carry, items):
        parts = front_pass(items[0], items[1], kernel)
        return (carry + lax.optimization_barrier(jnp.sum(parts[4] * parts[0], 0)), None)
    sum_first = lax.scan(mean_step, zeros_row, (pre_glu, lengths))[0]
    mean_value = sum_first / frame_total

    def spread_step(carry, items):
        parts = front_pass(items[0], items[1], kernel)
        centered = parts[4] - mean_value
        return (carry + lax.optimization_barrier(jnp.sum(centered * centered * parts[0], 0)), None)
    sum_square = lax.scan(spread_step, zeros_row, (pre_glu, lengths))[0]
    invstd = lax.rsqrt(sum_square / frame_total + epsilon)

    def act_parts(pre_one, length, cot_one):
        parts = front_pass(pre_one, length, kernel)
        normed = (parts[4] - mean_value) * invstd
        act_in = bn_gain * normed + bn_shift
        sig_act = jax.nn.sigmoid(act_in)
        swished = (act_in * sig_act).astype(jnp.bfloat16)
        masked_cot = cot_one * parts[0].astype(jnp.bfloat16)
        grad_swish = jnp.dot(masked_cot, w_out.T, preferred_element_type=jnp.float32)
        grad_act = grad_swish * sig_act * (1.0 + act_in * (1.0 - sig_act))
        return (parts, normed, swished, masked_cot, grad_act)

    def weight_step(carry, items):
        parts, normed, swished, masked_cot, grad_act = act_parts(items[0], items[1], items[2])
        weight_sum = carry[0] + jnp.dot(swished.T, masked_cot, preferred_element_type=jnp.float32)
        return ((weight_sum, carry[1] + lax.optimization_barrier(jnp.sum(grad_act, 0)), carry[2] + lax.optimization_barrier(jnp.sum(grad_act * normed, 0))), None)
    start_carry = (jnp.zeros((model_width, model_width), jnp.float32), zeros_row, zeros_row)
    weight_sum, sum_shift, sum_gain = lax.scan(weight_step, start_carry, (pre_glu, lengths, cotangent))[0]

    def input_step(carry, items):
        parts, normed, swished, masked_cot, grad_act = act_parts(items[0], items[1], items[2])
        valid_mask, first_half, gate_value, padded = (parts[0], parts[1], parts[2], parts[3])
        grad_conv = valid_mask * bn_gain * invstd * (grad_act - (sum_shift + normed * sum_gain) / frame_total)
        kernel_part = jnp.stack([lax.optimization_barrier(jnp.sum(grad_conv * padded[j:j + frames], 0)) for j in range(kernel_taps)], 0)
        grad_padded = jnp.pad(grad_conv, ((half_width, half_width), (0, 0)))
        grad_glu = kernel[0] * grad_padded[kernel_taps - 1:kernel_taps - 1 + frames]
        for j in range(1, kernel_taps):
            grad_glu = grad_glu + kernel[j] * grad_padded[kernel_taps - 1 - j:kernel_taps - 1 - j + frames]
        grad_glu = grad_glu * valid_mask
        grad_first = grad_glu * gate_value
        grad_second = grad_glu * first_half * gate_value * (1.0 - gate_value)
        grad_pre = jnp.concatenate([grad_first, grad_second], 1).astype(jnp.bfloat16)
        return (carry + kernel_part, grad_pre)
    kernel_sum, grad_pre_glu = lax.scan(input_step, jnp.zeros((kernel_taps, model_width), jnp.float32), (pre_glu, lengths, cotangent))
    return (grad_pre_glu, weight_sum / replicas, kernel_sum / replicas, sum_gain / replicas, sum_shift / replicas)
```

```python
import jax
import jax.numpy as jnp
from jax import lax
from jax.sharding import PartitionSpec as P

epsilon = 1e-05
AXES = ("dp", "local")


def factors_of(number):
    found = []
    factor = 2
    while number > 1:
        while number % factor == 0:
            found.append(factor)
            number //= factor
        factor += 1
    return found


class Digit:
    def __init__(self, size, stride, total):
        self.size, self.stride, self.total = size, stride, total

    def own(self, linear):
        return linear // self.stride % self.size

    def shift(self, value, step):
        def target(place):
            digit = place // self.stride % self.size
            return place + ((digit + step) % self.size - digit) * self.stride

        return lax.ppermute(value, AXES, [(place, target(place)) for place in range(self.total)])


def sum_over(value, digits):
    for digit in digits:
        parts = [digit.shift(value, step) for step in range(1, digit.size)]
        for part in parts:
            value = value + part
    return value


def scatter_over(value, axis, digit, linear):
    mine = digit.own(linear)
    received = []
    for step in range(1, digit.size):
        block = lax.dynamic_index_in_dim(value, (mine + step) % digit.size, axis, keepdims=True)
        received.append(digit.shift(block, step))
    total = lax.dynamic_index_in_dim(value, mine, axis, keepdims=True)
    for part in received:
        total = total + part
    return total


def taps_of(padded, kernel_taps, frames):
    return [padded[j : j + frames] for j in range(kernel_taps)]


def on_device(pre_glu, lengths, kernel, bn_gain, bn_shift, w_out, cotangent):
    frames = pre_glu.shape[1]
    model_width = kernel.shape[1]
    out_width = cotangent.shape[2]
    kernel_taps = kernel.shape[0]
    half_width = (kernel_taps - 1) // 2
    dp_size, local_size = lax.axis_size("dp"), lax.axis_size("local")
    replicas = dp_size * local_size
    linear = lax.axis_index("dp") * local_size + lax.axis_index("local")

    across = Digit(local_size, 1, replicas)
    pair = 2 if dp_size % 2 == 0 else 1
    core = Digit(pair, local_size, replicas)
    outer, stride = [], local_size * pair
    for factor in factors_of(dp_size // pair):
        outer.append(Digit(factor, stride, replicas))
        stride *= factor
    small_order = [core, *outer, across]

    valid_mask = (jnp.arange(frames, dtype=jnp.int32)[:, None] < lengths[0]).astype(jnp.float32)
    masked_cot = cotangent[0] * valid_mask.astype(jnp.bfloat16)
    my_core, my_across = core.own(linear), across.own(linear)
    piece = out_width // (local_size * pair)
    cot_pieces = cotangent[0].reshape(frames, local_size, pair, piece)
    other_cot = []
    for step in range(1, pair):
        sent = lax.dynamic_index_in_dim(cot_pieces, (my_core + step) % pair, 2, keepdims=False)
        other_cot.append(core.shift(sent.astype(jnp.float32), step))

    first_half = pre_glu[0, :, :model_width].astype(jnp.float32)
    gate_value = jax.nn.sigmoid(pre_glu[0, :, model_width:].astype(jnp.float32))
    glu_out = first_half * gate_value * valid_mask
    padded = jnp.pad(glu_out, ((half_width, half_width), (0, 0)))
    shifted = taps_of(padded, kernel_taps, frames)
    conv_out = kernel[0] * shifted[0]
    for j in range(1, kernel_taps):
        conv_out = conv_out + kernel[j] * shifted[j]
    masked_conv = conv_out * valid_mask
    stats = jnp.concatenate(
        [
            jnp.sum(masked_conv, 0),
            jnp.sum(conv_out * masked_conv, 0),
            jnp.full((128,), lengths[0].astype(jnp.float32)),
        ]
    )
    other_stats = [core.shift(stats, step) for step in range(1, pair)]
    for part in other_stats:
        stats = stats + part
    stats = sum_over(stats, small_order[1:])
    own_cot = masked_cot.reshape(cot_pieces.shape)
    pair_cot = [lax.dynamic_index_in_dim(own_cot, my_core, 2, keepdims=False)]
    for value, part in zip(other_cot, other_stats):
        other_mask = jnp.arange(frames)[:, None, None] < part[2 * model_width]
        pair_cot.append((value * other_mask.astype(jnp.float32)).astype(jnp.bfloat16))
    pair_cot = jnp.concatenate(pair_cot, 0)
    pair_conv = [conv_out] + [core.shift(conv_out, step) for step in range(1, pair)]

    frame_total = stats[2 * model_width]
    mean_value = stats[:model_width] / frame_total
    variance = stats[model_width : 2 * model_width] / frame_total - mean_value * mean_value
    invstd = lax.rsqrt(variance + epsilon)

    def activation(conv_one):
        normed = (conv_one - mean_value) * invstd
        act_in = bn_gain * normed + bn_shift
        return normed, act_in, jax.nn.sigmoid(act_in)

    pair_swished = []
    for conv_one in pair_conv:
        _, act_in, sig_act = activation(conv_one)
        pair_swished.append((act_in * sig_act).astype(jnp.bfloat16))
    pair_swished = jnp.concatenate(pair_swished, 0)

    colours = 3 if piece % 3 == 0 and len(outer) >= 2 else 1
    width = piece // colours
    rows = model_width // dp_size
    contract = (((0,), (0,)), ((), ()))
    digits = [across, *outer[:2]]
    axis_of = {id(across): len(outer) + 1}
    for place, digit in enumerate(outer):
        axis_of[id(digit)] = len(outer) - 1 - place
    partials = []
    for colour in range(colours):
        columns = pair_cot[:, :, colour * width : (colour + 1) * width]
        columns = columns.reshape(columns.shape[0], local_size * width)
        partial = lax.dot_general(
            pair_swished, columns, contract, preferred_element_type=jnp.float32
        )
        partial = partial.reshape(
            *[d.size for d in reversed(outer)], pair * rows, local_size, width
        )
        partials.append(partial)
    for turn in range(len(digits)):
        for colour in range(colours):
            digit = digits[(turn + colour) % len(digits)]
            partials[colour] = scatter_over(
                partials[colour], axis_of[id(digit)], digit, linear
            )
    merged = jnp.concatenate(partials, -1)
    for digit in outer[2:]:
        merged = scatter_over(merged, axis_of[id(digit)], digit, linear)
    merged = merged.reshape(pair, rows, piece)
    kept = lax.dynamic_index_in_dim(merged, my_core, 0, keepdims=False)
    halves = [kept]
    for step in range(1, pair):
        sent = lax.dynamic_index_in_dim(merged, (my_core + step) % pair, 0, keepdims=False)
        halves.append(core.shift(sent, step))
    if pair == 2:
        weight_shard = jnp.where(
            my_core == 0,
            jnp.concatenate(halves, 1),
            jnp.concatenate(halves[::-1], 1),
        )
    else:
        weight_shard = kept

    grad_swish = lax.dot_general(
        masked_cot, w_out, (((1,), (1,)), ((), ())), preferred_element_type=jnp.float32
    )
    normed, act_in, sig_act = activation(conv_out)
    grad_act = grad_swish * sig_act * (1.0 + act_in * (1.0 - sig_act))
    sums = [jnp.sum(grad_act, 0), jnp.sum(grad_act * normed, 0)]
    sums += [jnp.sum(grad_act * one, 0) for one in shifted]
    sums += [jnp.sum(valid_mask * one, 0) for one in shifted]
    sums += [jnp.sum(masked_conv * one, 0) for one in shifted]
    sums = sum_over(jnp.concatenate(sums), small_order).reshape(-1, model_width)
    sum_shift, sum_gain = sums[0], sums[1]
    act_taps = sums[2 : 2 + kernel_taps]
    plain_taps = sums[2 + kernel_taps : 2 + 2 * kernel_taps]
    conv_taps = sums[2 + 2 * kernel_taps :]
    channel_scale = bn_gain * invstd
    normed_taps = invstd * (conv_taps - mean_value * plain_taps)
    kernel_sum = channel_scale * (
        act_taps - (sum_shift * plain_taps + sum_gain * normed_taps) / frame_total
    )
    grad_conv = (
        valid_mask * channel_scale * (grad_act - (sum_shift + normed * sum_gain) / frame_total)
    )
    grad_padded = jnp.pad(grad_conv, ((half_width, half_width), (0, 0)))
    grad_glu = kernel[0] * grad_padded[kernel_taps - 1 : kernel_taps - 1 + frames]
    for j in range(1, kernel_taps):
        grad_glu = (
            grad_glu + kernel[j] * grad_padded[kernel_taps - 1 - j : kernel_taps - 1 - j + frames]
        )
    grad_glu = grad_glu * valid_mask
    grad_first = grad_glu * gate_value
    grad_second = grad_glu * first_half * gate_value * (1.0 - gate_value)
    grad_pre = jnp.concatenate([grad_first, grad_second], 1).astype(jnp.bfloat16)[None]
    return (
        grad_pre,
        weight_shard / replicas,
        kernel_sum / replicas,
        sum_gain / replicas,
        sum_shift / replicas,
    )


def solution(mesh):
    return jax.shard_map(
        on_device,
        mesh=mesh,
        in_specs=(
            P(("dp", "local"), None, None),
            P(("dp", "local")),
            P(),
            P(),
            P(),
            P(),
            P(("dp", "local"), None, None),
        ),
        out_specs=(P(("dp", "local"), None, None), P("dp", "local"), P(), P(), P()),
        check_vma=False,
    )
```

```python
import functools

import jax
import jax.numpy as jnp
from jax import lax
from jax.experimental import pallas as pl
from jax.experimental.pallas import tpu as pltpu
from jax.sharding import PartitionSpec as P


epsilon = 1e-05
AXES = ("dp", "local")
FRONT_PARAMS = pltpu.CompilerParams(vmem_limit_bytes=24 * 1024 * 1024)


def factors_of(number):
    found = []
    factor = 2
    while number > 1:
        while number % factor == 0:
            found.append(factor)
            number //= factor
        factor += 1
    return found


class Digit:
    def __init__(self, size, stride, total):
        self.size, self.stride, self.total = size, stride, total

    def locate(self, linear):
        mine = lax.rem(lax.div(linear, self.stride), self.size)
        self.places = [mine] + [
            lax.rem(mine + step, self.size) for step in range(1, self.size)
        ]
        return self.places

    def shift(self, value, step):
        def target(place):
            digit = place // self.stride % self.size
            return place + ((digit + step) % self.size - digit) * self.stride

        return lax.ppermute(value, AXES, [(place, target(place)) for place in range(self.total)])


def sum_over(value, digits):
    for digit in digits:
        parts = [digit.shift(value, step) for step in range(1, digit.size)]
        for part in parts:
            value = value + part
    return value


def block_of(value, place, axis):
    starts = [0] * value.ndim
    starts[axis] = place
    sizes = list(value.shape)
    sizes[axis] = 1
    return lax.dynamic_slice(value, starts, sizes, allow_negative_indices=False)


def scatter_over(value, axis, digit):
    received = []
    for step in range(1, digit.size):
        received.append(digit.shift(block_of(value, digit.places[step], axis), step))
    total = block_of(value, digit.places[0], axis)
    for part in received:
        total = total + part
    return total


def rows_below(frames, length):
    return lax.broadcasted_iota(jnp.int32, (frames, 1), 0) < length


def shift_rows(value, offset):
    frames = value.shape[0]
    if offset == 0:
        return value
    place = lax.broadcasted_iota(jnp.int32, (frames, 1), 0) + offset
    inside = jnp.logical_and(place >= 0, place < frames)
    return jnp.where(inside, pltpu.roll(value, (-offset) % frames, 0), 0.0)


def gated(first_ref, second_ref, mask):
    first_half = first_ref[0].astype(jnp.float32)
    gate_value = jax.nn.sigmoid(second_ref[0].astype(jnp.float32))
    return first_half, gate_value, first_half * gate_value * mask


def moments(stats_ref):
    frame_total = stats_ref[2:3]
    mean_value = stats_ref[0:1] / frame_total
    variance = stats_ref[1:2] / frame_total - mean_value * mean_value
    return frame_total, mean_value, lax.rsqrt(variance + epsilon)


def front_kernel(length_ref, first_ref, second_ref, taps_ref, conv_ref, stats_ref):
    frames = conv_ref.shape[0]
    kernel_taps = taps_ref.shape[0]
    mask = rows_below(frames, length_ref[0]).astype(jnp.float32)
    _, _, glu_out = gated(first_ref, second_ref, mask)
    conv_out = taps_ref[0:1] * shift_rows(glu_out, -(kernel_taps // 2))
    for j in range(1, kernel_taps):
        conv_out = conv_out + taps_ref[j : j + 1] * shift_rows(glu_out, j - kernel_taps // 2)
    conv_ref[...] = conv_out
    masked = conv_out * mask
    stats_ref[0:1] = jnp.sum(masked, 0, keepdims=True)
    stats_ref[1:2] = jnp.sum(conv_out * masked, 0, keepdims=True)
    count = jnp.full((1, conv_ref.shape[1]), length_ref[0], jnp.int32)
    stats_ref[2:3] = count.astype(jnp.float32)


def cot_kernel(places, step, scalar_ref, cot_ref, out_ref):
    pair, local_size, piece = places
    for place in range(local_size):
        start = pl.multiple_of((place * pair + scalar_ref[1 + step]) * piece, 128)
        out_ref[:, place * piece : (place + 1) * piece] = cot_ref[0, :, pl.ds(start, piece)].astype(
            jnp.float32
        )


def product_kernel(
    places, colours, scalar_ref, stats_ref, gain_ref, shift_ref, conv_ref, *refs
):
    pair, local_size, piece = places
    others, refs = refs[: pair - 1], refs[pair - 1 :]
    other_stats, refs = refs[: pair - 1], refs[pair - 1 :]
    cot_ref, refs = refs[0], refs[1:]
    other_cots, refs = refs[: pair - 1], refs[pair - 1 :]
    outs, right = refs[:-1], refs[-1]
    frames = conv_ref.shape[0]
    width = piece // colours

    @pl.when(pl.program_id(0) == 0)
    def _():
        for turn in range(pair):
            if turn == 0:
                mask = rows_below(frames, scalar_ref[0]).astype(jnp.float32)
            else:
                row = lax.broadcasted_iota(jnp.int32, (frames, width), 0).astype(jnp.float32)
                mask = (row < other_stats[turn - 1][2:3, :width]).astype(jnp.float32)
            for colour in range(colours):
                for place in range(local_size):
                    at = place * piece + colour * width
                    if turn == 0:
                        start = (place * pair + scalar_ref[1]) * piece + colour * width
                        value = cot_ref[0, :, pl.ds(pl.multiple_of(start, 128), width)]
                        value = value.astype(jnp.float32)
                    else:
                        value = other_cots[turn - 1][:, at : at + width]
                    to = (colour * local_size + place) * width
                    right[turn * frames : (turn + 1) * frames, to : to + width] = (
                        value * mask
                    ).astype(jnp.bfloat16)

    _, mean_value, invstd = moments(stats_ref)
    left = []
    for ref in (conv_ref, *others):
        act_in = gain_ref[...] * ((ref[...] - mean_value) * invstd) + shift_ref[...]
        left.append((act_in * jax.nn.sigmoid(act_in)).astype(jnp.bfloat16))
    left = jnp.concatenate(left, 0)
    for colour in range(colours):
        span = local_size * width
        both = lax.dot_general(
            left,
            right[:, colour * span : (colour + 1) * span],
            (((0,), (0,)), ((), ())),
            preferred_element_type=jnp.float32,
        )
        for place in range(local_size):
            outs[colour][place] = both[:, place * width : (place + 1) * width]


def grad_kernel(
    length_ref, stats_ref, gain_ref, shift_ref, conv_ref, first_ref, second_ref, cot_ref,
    weight_ref, grad_ref, sums_ref, cot_scratch, *, kernel_taps,
):
    frames = conv_ref.shape[0]
    mask = rows_below(frames, length_ref[0]).astype(jnp.float32)

    @pl.when(pl.program_id(0) == 0)
    def _():
        cot_scratch[...] = cot_ref[0] * mask.astype(jnp.bfloat16)

    _, _, glu_out = gated(first_ref, second_ref, mask)
    _, mean_value, invstd = moments(stats_ref)
    conv_out = conv_ref[...]
    normed = (conv_out - mean_value) * invstd
    act_in = gain_ref[...] * normed + shift_ref[...]
    sig_act = jax.nn.sigmoid(act_in)
    grad_swish = lax.dot_general(
        cot_scratch[...], weight_ref[...], (((1,), (1,)), ((), ())),
        preferred_element_type=jnp.float32,
    )
    grad_act = grad_swish * sig_act * (1.0 + act_in * (1.0 - sig_act))
    grad_ref[...] = grad_act
    masked = conv_out * mask
    sums_ref[0:1] = jnp.sum(grad_act, 0, keepdims=True)
    sums_ref[1:2] = jnp.sum(grad_act * normed, 0, keepdims=True)
    for j in range(kernel_taps):
        shifted = shift_rows(glu_out, j - kernel_taps // 2)
        for turn, value in enumerate((grad_act, mask, masked)):
            row = 2 + turn * kernel_taps + j
            sums_ref[row : row + 1] = jnp.sum(value * shifted, 0, keepdims=True)


def final_kernel(
    replicas, length_ref, stats_ref, sums_ref, gain_ref, taps_ref, conv_ref, first_ref,
    second_ref, grad_ref, pre_ref, taps_out, gain_out, shift_out,
):
    frames, width = conv_ref.shape
    kernel_taps = taps_ref.shape[0]
    mask = rows_below(frames, length_ref[0]).astype(jnp.float32)
    frame_total, mean_value, invstd = moments(stats_ref)
    sum_shift, sum_gain = sums_ref[0:1], sums_ref[1:2]
    scale = gain_ref[...] * invstd
    normed = (conv_ref[...] - mean_value) * invstd
    grad_conv = mask * scale * (grad_ref[...] - (sum_shift + normed * sum_gain) / frame_total)
    grad_glu = taps_ref[0:1] * shift_rows(grad_conv, kernel_taps // 2)
    for j in range(1, kernel_taps):
        grad_glu = grad_glu + taps_ref[j : j + 1] * shift_rows(grad_conv, kernel_taps // 2 - j)
    grad_glu = grad_glu * mask
    first_half, gate_value, _ = gated(first_ref, second_ref, mask)
    at = pl.multiple_of(pl.program_id(0) * width, 128)
    total = pl.num_programs(0) * width
    grad_first = grad_glu * gate_value
    pre_ref[0, :, pl.ds(at, width)] = grad_first.astype(jnp.bfloat16)
    grad_second = grad_glu * first_half * gate_value * (1.0 - gate_value)
    pre_ref[0, :, pl.ds(pl.multiple_of(total + at, 128), width)] = grad_second.astype(
        jnp.bfloat16
    )
    for j in range(kernel_taps):
        act_tap = sums_ref[2 + j : 3 + j]
        plain = sums_ref[2 + kernel_taps + j : 3 + kernel_taps + j]
        conv_tap = sums_ref[2 + 2 * kernel_taps + j : 3 + 2 * kernel_taps + j]
        normed_tap = invstd * (conv_tap - mean_value * plain)
        taps_out[j : j + 1] = (
            scale * (act_tap - (sum_shift * plain + sum_gain * normed_tap) / frame_total)
        ) / replicas
    gain_out[...] = sum_gain / replicas
    shift_out[...] = sum_shift / replicas


def one_device(pre_glu, lengths, kernel, bn_gain, bn_shift, w_out, cotangent):
    frames = pre_glu.shape[1]
    model_width = kernel.shape[1]
    out_width = cotangent.shape[2]
    kernel_taps = kernel.shape[0]
    dp_size, local_size = lax.axis_size("dp"), lax.axis_size("local")
    replicas = dp_size * local_size
    linear = lax.axis_index("dp") * local_size + lax.axis_index("local")

    across = Digit(local_size, 1, replicas)
    pair = 2 if dp_size % 2 == 0 else 1
    core = Digit(pair, local_size, replicas)
    outer, stride = [], local_size * pair
    for factor in factors_of(dp_size // pair):
        outer.append(Digit(factor, stride, replicas))
        stride *= factor
    places = []
    for digit in [core, across, *outer]:
        places += digit.locate(linear.astype(jnp.int32))
    scalars = jnp.stack([lengths[0], *places])
    my_core = core.places[0]
    piece = out_width // (local_size * pair)
    gain_row, shift_row = bn_gain[None], bn_shift[None]

    block = 256 if model_width % 256 == 0 else model_width
    steps = model_width // block
    smem = pl.BlockSpec(memory_space=pltpu.SMEM)

    def columns(height):
        return pl.BlockSpec((height, block), lambda c: (0, c))

    halves = [
        pl.BlockSpec((1, frames, block), lambda c: (0, 0, c)),
        pl.BlockSpec((1, frames, block), lambda c: (0, 0, c + steps)),
    ]
    params = pltpu.CompilerParams(vmem_limit_bytes=24 * 1024 * 1024)
    wide = jax.ShapeDtypeStruct((frames, model_width), jnp.float32)

    conv_out, stats = pl.pallas_call(
        front_kernel,
        grid=(steps,),
        in_specs=[smem, *halves, columns(kernel_taps)],
        out_specs=[columns(frames), columns(3)],
        out_shape=[wide, jax.ShapeDtypeStruct((3, model_width), jnp.float32)],
        compiler_params=FRONT_PARAMS,
    )(scalars, pre_glu, pre_glu, kernel)
    sent_cots = []
    for step in range(1, pair):
        sent_cots.append(
            pl.pallas_call(
                functools.partial(cot_kernel, (pair, local_size, piece), step),
                in_specs=[smem, pl.BlockSpec(memory_space=pltpu.VMEM)],
                out_specs=pl.BlockSpec(memory_space=pltpu.VMEM),
                out_shape=jax.ShapeDtypeStruct((frames, local_size * piece), jnp.float32),
                compiler_params=params,
            )(scalars, cotangent)
        )

    other_cots = []
    for step in range(1, pair):
        other_cots.append(core.shift(sent_cots[step - 1], step))

    other_stats = [core.shift(stats, step) for step in range(1, pair)]
    other_convs = [core.shift(conv_out, step) for step in range(1, pair)]
    for part in other_stats:
        stats = stats + part
    stats = sum_over(stats, [*outer, across])

    colours = 3 if piece % 3 == 0 and len(outer) >= 2 else 1
    width = piece // colours
    rows = model_width // dp_size
    left_block = 384 if model_width % 384 == 0 else model_width

    def left_columns(height):
        return pl.BlockSpec((height, left_block), lambda c: (0, c))

    span = local_size * width
    partials = pl.pallas_call(
        functools.partial(product_kernel, (pair, local_size, piece), colours),
        grid=(model_width // left_block,),
        in_specs=[smem, left_columns(3), left_columns(1), left_columns(1)]
        + [left_columns(frames)] * pair
        + [pl.BlockSpec((3, model_width), lambda c: (0, 0))] * (pair - 1)
        + [pl.BlockSpec((1, frames, out_width), lambda c: (0, 0, 0))]
        + [pl.BlockSpec((frames, local_size * piece), lambda c: (0, 0))] * (pair - 1),
        out_specs=[pl.BlockSpec((local_size, left_block, width), lambda c: (0, c, 0))] * colours,
        out_shape=[
            jax.ShapeDtypeStruct((local_size, model_width, width), jnp.float32)
        ]
        * colours,
        scratch_shapes=[pltpu.VMEM((pair * frames, colours * span), jnp.bfloat16)],
        compiler_params=params,
    )(
        scalars, stats, gain_row, shift_row, conv_out, *other_convs, *other_stats,
        cotangent, *other_cots,
    )
    partials = [
        value.reshape(local_size, *[d.size for d in reversed(outer)], pair * rows, width)
        for value in partials
    ]

    digits = [across, *outer[:2]]
    axis_of = {id(across): 0}
    for place, digit in enumerate(outer):
        axis_of[id(digit)] = len(outer) - place
    for turn in range(len(digits)):
        for colour in range(colours):
            digit = digits[(turn + colour) % len(digits)]
            partials[colour] = scatter_over(
                partials[colour], axis_of[id(digit)], digit
            )
    merged = jnp.concatenate(partials, -1)
    for digit in outer[2:]:
        merged = scatter_over(merged, axis_of[id(digit)], digit)
    merged = merged.reshape(pair, rows, piece)
    kept = block_of(merged, my_core, 0)[0]
    pieces = [kept]
    for step in range(1, pair):
        sent = block_of(merged, core.places[step], 0)[0]
        pieces.append(core.shift(sent, step))
    if pair == 2:
        weight_shard = jnp.where(
            my_core == 0,
            jnp.concatenate(pieces, 1),
            jnp.concatenate(pieces[::-1], 1),
        )
    else:
        weight_shard = kept

    height = 2 + 3 * kernel_taps
    grad_act, sums = pl.pallas_call(
        functools.partial(grad_kernel, kernel_taps=kernel_taps),
        grid=(steps,),
        in_specs=[smem, columns(3), columns(1), columns(1), columns(frames), *halves]
        + [
            pl.BlockSpec((1, frames, out_width), lambda c: (0, 0, 0)),
            pl.BlockSpec((block, out_width), lambda c: (c, 0)),
        ],
        out_specs=[columns(frames), columns(height)],
        out_shape=[wide, jax.ShapeDtypeStruct((height, model_width), jnp.float32)],
        scratch_shapes=[pltpu.VMEM((frames, out_width), jnp.bfloat16)],
        compiler_params=params,
    )(scalars, stats, gain_row, shift_row, conv_out, pre_glu, pre_glu, cotangent, w_out)
    sums = sum_over(sums, [core, across, *outer])
    row = jax.ShapeDtypeStruct((1, model_width), jnp.float32)
    grad_pre, kernel_grad, gain_grad, shift_grad = pl.pallas_call(
        functools.partial(final_kernel, float(replicas)),
        grid=(steps,),
        in_specs=[smem, columns(3), columns(height), columns(1), columns(kernel_taps)]
        + [columns(frames), *halves, columns(frames)],
        out_specs=[
            pl.BlockSpec((1, frames, 2 * model_width), lambda c: (0, 0, 0)),
            columns(kernel_taps),
            columns(1),
            columns(1),
        ],
        out_shape=[
            jax.ShapeDtypeStruct((1, frames, 2 * model_width), jnp.bfloat16),
            jax.ShapeDtypeStruct((kernel_taps, model_width), jnp.float32),
            row,
            row,
        ],
        compiler_params=params,
    )(scalars, stats, sums, gain_row, kernel, conv_out, pre_glu, pre_glu, grad_act)
    return (
        grad_pre,
        weight_shard / replicas,
        kernel_grad,
        gain_grad.reshape(model_width),
        shift_grad.reshape(model_width),
    )


def solution(mesh):
    return jax.shard_map(
        one_device,
        mesh=mesh,
        in_specs=(
            P(("dp", "local"), None, None),
            P(("dp", "local")),
            P(),
            P(),
            P(),
            P(),
            P(("dp", "local"), None, None),
        ),
        out_specs=(P(("dp", "local"), None, None), P("dp", "local"), P(), P(), P()),
        check_vma=False,
    )
```
